128 devices in a mesh: sector: 16 (over y, x_lo, core), row: 8 (over z, x_hi).
Axes of the slice: x: 4 (x_hi: 2, x_lo: 2; x = x_hi * 2 + x_lo), y: 4, z: 4, core: 2. Of those that a mesh axis runs over, the one named last changes fastest.
Arguments:
- psi_sectors: bfloat16 [64, 16384, 256], P('sector', 'row'), may hold values from -1.25 to 1.25
- stiff_blocks: bfloat16 [128, 5, 128, 128], P('row'), as said below
- mass_blocks: bfloat16 [128, 5, 128, 128], P('row'), as said below
- harmonic_table: int32 [32], replicated, may hold values from 0 to 31, each once
Outputs:
- reduced_stiffness: float32 [32, 512, 512], P('sector', 'row')
- reduced_mass: float32 [32, 512, 512], P('sector', 'row')
The draws below stay inside these ranges and needn't reach their ends.
Inputs may be any that keep to these rules, and one draw needn't show every extreme that they name: The stiffness is symmetric: stiff_blocks[i, 2 + d] is the transpose of stiff_blocks[i + d, 2 - d], and blocks whose column lies outside 0 to 127 are zero. `mass_blocks`: the mass is symmetric in the same way, and diagonally dominant with a positive diagonal, hence positive definite.
All inputs are finite; a program needn't handle non-finite values.
Results may differ from the reference program's by a relative error of at most 0.0049.
Values may be sent and summed in bfloat16 or wider, within the bound.
No kernel may reach another device: no remote copies, remote signals or barrier semaphores. Data moves between devices by JAX's collectives and lax.ppermute only.
A program may use at most 128 MiB of HBM per device.

```python
import math
import jax
import jax.numpy as jnp
from jax import lax

M = 256
B = 128
REACH = 2
NBAND = 5
SECTORS = 64
SLOTS = 32
DOF = 16384
NBLK = 128


def build_band(key, entry_scale):
    upper_part = jnp.clip(jax.random.normal(key, (NBLK, REACH + 1, B, B), jnp.float32), -6.0, 6.0) * entry_scale
    middle = (upper_part[:, 0] + jnp.swapaxes(upper_part[:, 0], 1, 2)) * 0.5 ** 0.5
    block_ids = jnp.arange(NBLK, dtype=jnp.int32)[:, None, None]
    columns = []
    for offset in range(-REACH, REACH + 1):
        if offset == 0:
            columns.append(middle)
        elif offset > 0:
            inside = block_ids + offset < NBLK
            columns.append(jnp.where(inside, upper_part[:, offset], 0.0))
        else:
            distance = -offset
            flipped = jnp.swapaxes(upper_part[:, distance], 1, 2)
            shifted = jnp.concatenate([jnp.zeros((distance, B, B), jnp.float32), flipped[:NBLK - distance]], axis=0)
            columns.append(shifted)
    return jnp.stack(columns, axis=1)


def draw_stiff_blocks(key, part):
    band = build_band(jax.random.fold_in(key, 11), (NBAND * B) ** (-0.5))
    return band.astype(jnp.bfloat16)


def draw_mass_blocks(key, part):
    band = build_band(jax.random.fold_in(key, 23), 1.0 / (NBAND * B))
    identity = jnp.eye(B, dtype=jnp.float32)
    own_diagonal = jnp.abs(jnp.diagonal(band[:, REACH], axis1=1, axis2=2))
    off_sum = jnp.sum(jnp.abs(band), axis=(1, 3)) - own_diagonal
    factor = jax.random.uniform(jax.random.fold_in(key, 29), (NBLK, B), jnp.float32, 1.1, 2.0)
    new_diagonal = off_sum * factor
    centre = band[:, REACH] * (1.0 - identity) + new_diagonal[:, :, None] * identity
    band = band.at[:, REACH].set(centre)
    return band.astype(jnp.bfloat16)


def block_scale(key, dims, cuts, smallest, largest):
    level = 1.0
    for position, parts in cuts:
        steps = jax.random.uniform(jax.random.fold_in(jax.random.fold_in(key, 6), position), (parts,), jnp.float32, smallest / len(cuts), largest / len(cuts))
        level = level * jnp.repeat(jnp.exp(steps), dims[position] // parts).reshape((-1,) + (1,) * (len(dims) - 1 - position))
    return level


def gaussian(rng, extent, spread, reach, split=(), kind=jnp.bfloat16):
    entries = jax.random.normal(rng, extent, jnp.float32) * spread
    if len(split) > 0:
        entries = block_scale(rng, extent, split, -0.22, 0.18) * entries
    return jnp.clip(entries, min=-reach, max=reach).astype(kind)


def setup_inputs(seed: int = 0) -> dict:
    streams_of = jax.random.split(jax.random.key(seed), 5)
    return {
        "psi_sectors": gaussian(streams_of[0], (SECTORS, DOF, M), (DOF ** -0.25), 1.25, ((0, 16), (1, 8))),
        "stiff_blocks": draw_stiff_blocks(jax.random.fold_in(streams_of[4], 71), 0),
        "mass_blocks": draw_mass_blocks(jax.random.fold_in(streams_of[4], 71), 0),
        "harmonic_table": jax.random.permutation(streams_of[3], SLOTS).astype(jnp.int32),
    }


def coefficients(harmonic_table, sectors_all):
    sector_ids = jnp.arange(sectors_all, dtype=jnp.int32)
    pair_table = harmonic_table.astype(jnp.int32)
    half_count = sectors_all // 2
    second_freq = jnp.where(pair_table == 0, half_count, pair_table)
    first_phase = pair_table[:, None] * sector_ids[None, :] % sectors_all
    second_phase = second_freq[:, None] * sector_ids[None, :] % sectors_all
    angle_unit = 2.0 * math.pi / sectors_all
    first_angle = first_phase.astype(jnp.float32) * angle_unit
    second_angle = second_phase.astype(jnp.float32) * angle_unit
    zero_pair = (pair_table == 0)[:, None]
    low_scale = math.sqrt(1.0 / sectors_all)
    high_scale = math.sqrt(2.0 / sectors_all)
    first_row = jnp.where(zero_pair, low_scale, high_scale) * jnp.cos(first_angle)
    second = jnp.where(zero_pair, low_scale * jnp.cos(second_angle), high_scale * jnp.sin(second_angle))
    return jnp.stack([first_row, second], axis=1).reshape(2 * pair_table.shape[0], sectors_all)

def band_apply(blocks, harmonic):
    block_rows = blocks.shape[0]
    band_count = blocks.shape[1]
    padded = jnp.pad(harmonic.reshape(block_rows, B, harmonic.shape[1]), ((REACH, REACH), (0, 0), (0, 0)))
    block_index = jnp.arange(block_rows, dtype=jnp.int32)[:, None] + jnp.arange(band_count, dtype=jnp.int32)[None, :]
    gathered = padded[block_index].astype(jnp.float32)
    images = jnp.einsum('ijab,ijbm->iam', blocks.astype(jnp.float32), gathered)
    return images.reshape(harmonic.shape).astype(jnp.bfloat16)

def reference(psi_sectors, stiff_blocks, mass_blocks, harmonic_table):
    sectors_all = psi_sectors.shape[0]
    dof_count = psi_sectors.shape[1]
    mode_count = psi_sectors.shape[2]
    dft_table = coefficients(harmonic_table, sectors_all)
    flattened = psi_sectors.reshape(sectors_all, dof_count * mode_count).astype(jnp.float32)
    harmonics = jnp.dot(dft_table, flattened, precision=lax.Precision.HIGHEST).astype(jnp.bfloat16)
    harmonics = harmonics.reshape(sectors_all // 2, 2, dof_count, mode_count)

    def one_slot(pair_field):
        left_basis = jnp.concatenate([pair_field[0], pair_field[1]], axis=1)
        stiff_wide = jnp.concatenate([band_apply(stiff_blocks, pair_field[0]), band_apply(stiff_blocks, pair_field[1])], axis=1)
        mass_wide = jnp.concatenate([band_apply(mass_blocks, pair_field[0]), band_apply(mass_blocks, pair_field[1])], axis=1)
        return (jnp.dot(left_basis.T, stiff_wide, preferred_element_type=jnp.float32), jnp.dot(left_basis.T, mass_wide, preferred_element_type=jnp.float32))
    reduced_stiffness, reduced_mass = lax.map(one_slot, harmonics)
    return (reduced_stiffness, reduced_mass)
```

```python
import math

import jax
import jax.numpy as jnp
from jax import lax
from jax.experimental import pallas as pl
from jax.experimental.pallas import tpu as pltpu
from jax.sharding import PartitionSpec as P

B = 128
REACH = 2
LANES = 256
STEP_ROWS = 16


def slot_of_harmonic(harmonic_table):
    slots = jnp.arange(harmonic_table.shape[0], dtype=jnp.int32)
    hit = harmonic_table[:, None] == slots[None, :]
    return jnp.sum(jnp.where(hit, slots[:, None], 0), axis=0)


def real_dft8(x):
    half = math.sqrt(0.5)
    s0, d0 = x[0] + x[4], x[0] - x[4]
    s1, d1 = x[2] + x[6], x[2] - x[6]
    s2, d2 = x[1] + x[5], x[1] - x[5]
    s3, d3 = x[3] + x[7], x[3] - x[7]
    e0, e2 = s0 + s1, s0 - s1
    o0, o2 = s2 + s3, s2 - s3
    t_re, t_im = (d2 - d3) * half, (d2 + d3) * half
    return [
        (e0 + o0, None),
        (d0 + t_re, d1 + t_im),
        (e2, o2),
        (d0 - t_re, t_im - d1),
        (e0 - o0, None),
    ]


def dft4(a, b, c, d):
    s0, d0 = (a[0] + c[0], a[1] + c[1]), (a[0] - c[0], a[1] - c[1])
    s1, d1 = (b[0] + d[0], b[1] + d[1]), (b[0] - d[0], b[1] - d[1])
    return [
        (s0[0] + s1[0], s0[1] + s1[1]),
        (d0[0] - d1[1], d0[1] + d1[0]),
        (s0[0] - s1[0], s0[1] - s1[1]),
        (d0[0] + d1[1], d0[1] - d1[0]),
    ]


def complex_dft8(z):
    half = math.sqrt(0.5)
    even = dft4(z[0], z[2], z[4], z[6])
    odd = dft4(z[1], z[3], z[5], z[7])
    turned = [
        odd[0],
        ((odd[1][0] - odd[1][1]) * half, (odd[1][0] + odd[1][1]) * half),
        (-odd[2][1], odd[2][0]),
        (-(odd[3][0] + odd[3][1]) * half, (odd[3][0] - odd[3][1]) * half),
    ]
    low = [(e[0] + t[0], e[1] + t[1]) for e, t in zip(even, turned)]
    high = [(e[0] - t[0], e[1] - t[1]) for e, t in zip(even, turned)]
    return low + high


def transform_kernel(slot_ref, x_ref, out_ref, mid_ref):
    sectors = 64
    scale = math.sqrt(2.0 / sectors)

    def put(p, re, im):
        at = 2 * slot_ref[p]
        return at, re, im

    for tile in range(STEP_ROWS // 8):
        rows = slice(8 * tile, 8 * tile + 8)

        def store(c, value):
            out_ref[c, rows, :] = value.astype(jnp.bfloat16)

        for s0 in range(8):
            x = []
            for s1 in range(8):
                s = 8 * s1 + s0
                x.append(x_ref[s // 4, s % 4, rows, :].astype(jnp.float32))
            y = real_dft8(x)
            mid_ref[tile, 0, s0] = y[0][0]
            mid_ref[tile, 1, s0] = y[4][0]
            for k1 in range(1, 4):
                mid_ref[tile, 2 * k1, s0] = y[k1][0]
                mid_ref[tile, 2 * k1 + 1, s0] = y[k1][1]
        y = real_dft8([mid_ref[tile, 0, s0] for s0 in range(8)])
        at = 2 * slot_ref[0]
        store(at, y[0][0] * math.sqrt(1.0 / sectors))
        store(at + 1, y[4][0] * math.sqrt(1.0 / sectors))
        for k2 in range(1, 4):
            at = 2 * slot_ref[8 * k2]
            store(at, y[k2][0] * scale)
            store(at + 1, y[k2][1] * scale)
        z = []
        for s0 in range(8):
            angle = 2.0 * math.pi * 4 * s0 / sectors
            value = mid_ref[tile, 1, s0]
            z.append((value * (scale * math.cos(angle)), value * (scale * math.sin(angle))))
        y = complex_dft8(z)
        for k2 in range(4):
            at = 2 * slot_ref[4 + 8 * k2]
            store(at, y[k2][0])
            store(at + 1, y[k2][1])
        for k1 in range(1, 4):
            z = []
            for s0 in range(8):
                angle = 2.0 * math.pi * k1 * s0 / sectors
                c, s = scale * math.cos(angle), scale * math.sin(angle)
                re, im = mid_ref[tile, 2 * k1, s0], mid_ref[tile, 2 * k1 + 1, s0]
                z.append((re * c, im * c) if s0 == 0 else (re * c - im * s, re * s + im * c))
            y = complex_dft8(z)
            for k2 in range(8):
                p = k1 + 8 * k2
                if p < 32:
                    at = 2 * slot_ref[p]
                    store(at, y[k2][0])
                    store(at + 1, y[k2][1])
                else:
                    at = 2 * slot_ref[64 - p]
                    store(at, y[k2][0])
                    store(at + 1, -y[k2][1])


def transform(slots, arrived):
    groups, per, rows, cols = arrived.shape
    spec = pltpu.PrefetchScalarGridSpec(
        num_scalar_prefetch=1,
        grid=(rows // STEP_ROWS,),
        in_specs=[pl.BlockSpec((groups, per, STEP_ROWS, cols), lambda i, s: (0, 0, i, 0))],
        out_specs=pl.BlockSpec((groups * per, STEP_ROWS, cols), lambda i, s: (0, i, 0)),
        scratch_shapes=[pltpu.VMEM((STEP_ROWS // 8, 8, 8, 8, cols), jnp.float32)],
    )
    return pl.pallas_call(
        transform_kernel,
        grid_spec=spec,
        out_shape=jax.ShapeDtypeStruct((groups * per, rows, cols), jnp.bfloat16),
        compiler_params=pltpu.CompilerParams(dimension_semantics=("arbitrary",)),
        cost_estimate=pl.CostEstimate(
            flops=700 * rows * cols, bytes_accessed=4 * groups * per * rows * cols, transcendentals=0
        ),
        name="transform",
    )(slots, arrived)


def project_kernel(h_ref, halo_ref, stiff_ref, mass_ref, out_ref, y_ref, pt_ref, u_ref):
    blocks = h_ref.shape[0]
    slots = h_ref.shape[1] // 2

    def window(refs_rows):
        return jnp.concatenate(refs_rows, axis=0)

    def band_row(i, h0, h1, h2):
        rows = pl.ds(i * B, B)
        lhs = jnp.concatenate(
            [
                jnp.concatenate([r[i, 2] * jnp.bfloat16(0.5), r[i, 3], r[i, 4]], axis=1)
                for r in (stiff_ref, mass_ref)
            ],
            axis=0,
        )
        for c in range(2 * slots):
            rhs = jnp.concatenate([h0[c], h1[c], h2[c]], axis=0)
            y = jnp.dot(lhs, rhs, preferred_element_type=jnp.float32).astype(jnp.bfloat16)
            slot, part = c // 2, c % 2
            lanes = slice(LANES * part, LANES * part + LANES)
            lanes_m = slice(LANES * (2 + part), LANES * (2 + part) + LANES)
            y_ref[slot, rows, lanes] = y[:B]
            y_ref[slot, rows, lanes_m] = y[B:]
            pt_ref[slot, i, LANES * part : LANES * part + LANES, :] = h0[c].T

    def body(i, carry):
        band_row(i, h_ref.at[i], h_ref.at[i + 1], h_ref.at[i + 2])
        return carry

    lax.fori_loop(0, blocks - 2, body, 0)
    band_row(blocks - 2, h_ref.at[blocks - 2], h_ref.at[blocks - 1], halo_ref.at[0])
    band_row(blocks - 1, h_ref.at[blocks - 1], halo_ref.at[0], halo_ref.at[1])

    for slot in range(slots):
        p_t = jnp.concatenate([pt_ref[slot, i] for i in range(blocks)], axis=1)
        for n in range(4):
            u_ref[slot, :, LANES * n : LANES * n + LANES] = jnp.dot(
                p_t, y_ref[slot, :, LANES * n : LANES * n + LANES], preferred_element_type=jnp.float32
            )
    strips = out_ref.shape[0]
    high = out_ref.shape[2]
    for kind in range(2):
        for slot in range(slots):
            base = 2 * LANES * kind
            for q in range(4):
                direct = u_ref[slot, B * q : B * q + B, base : base + 2 * LANES]
                mirror = u_ref[slot, :, base + B * q : base + B * q + B].T
                total = (direct + mirror).astype(jnp.bfloat16)
                for part in range(B // high):
                    out_ref[q * (B // high) + part, kind * slots + slot] = total[
                        part * high : (part + 1) * high
                    ]


def project(h, halo, stiff, mass, strips):
    blocks, comps, _, cols = h.shape
    slots = comps // 2
    wide = 2 * cols
    vmem = pl.BlockSpec(memory_space=pltpu.VMEM)
    return pl.pallas_call(
        project_kernel,
        in_specs=[vmem] * 4,
        out_specs=vmem,
        out_shape=jax.ShapeDtypeStruct((strips, 2 * slots, wide // strips, wide), jnp.bfloat16),
        scratch_shapes=[
            pltpu.VMEM((slots, blocks * B, 2 * wide), jnp.bfloat16),
            pltpu.VMEM((slots, blocks, wide, B), jnp.bfloat16),
            pltpu.VMEM((slots, wide, 2 * wide), jnp.float32),
        ],
        compiler_params=pltpu.CompilerParams(vmem_limit_bytes=48 * 1024 * 1024),
        cost_estimate=pl.CostEstimate(
            flops=slots * blocks * B * wide * (2 * 2 * 3 * B + 2 * 2 * wide),
            bytes_accessed=2 * (h.size + halo.size + stiff.size + mass.size),
            transcendentals=0,
        ),
        name="project",
    )(h, halo, stiff, mass)


def per_device(psi_sectors, stiff_blocks, mass_blocks, harmonic_table):
    sec_dev, rows_dev, cols = psi_sectors.shape
    sector_count = lax.axis_size("sector")
    row_count = lax.axis_size("row")
    blocks = rows_dev // B
    pieces = psi_sectors.reshape(sec_dev, sector_count, rows_dev // sector_count, cols)
    pieces = jnp.swapaxes(pieces, 0, 1)
    arrived = lax.all_to_all(pieces, "sector", 0, 0, tiled=True)
    components = transform(slot_of_harmonic(harmonic_table), arrived)
    outgoing = components.reshape(sector_count, sec_dev, rows_dev // sector_count, cols)
    h = lax.all_to_all(outgoing, "sector", 0, 0, tiled=True)
    h = h.reshape(sector_count, sec_dev, -1, B, cols)
    h = jnp.swapaxes(h, 1, 2).reshape(blocks, sec_dev, B, cols)
    backward = [(i + 1, i) for i in range(row_count - 1)]
    halo = lax.ppermute(h[:REACH], "row", backward)
    parts = project(h, halo, stiff_blocks, mass_blocks, row_count)
    arrived_parts = lax.all_to_all(parts, "row", 0, 0, tiled=True)
    total = jnp.sum(arrived_parts.astype(jnp.float32), axis=0)
    slots = sec_dev // 2
    return total[:slots], total[slots:]


def solution(mesh):
    placed = (P("sector", "row", None), P("row", None, None, None), P("row", None, None, None), P())
    return jax.shard_map(
        per_device,
        mesh=mesh,
        in_specs=placed,
        out_specs=(P("sector", "row", None), P("sector", "row", None)),
        check_vma=False,
    )
```

```python
import math

import jax
import jax.numpy as jnp
from jax import lax
from jax.experimental import pallas as pl
from jax.experimental.pallas import tpu as pltpu
from jax.sharding import PartitionSpec as P

B = 128
REACH = 2
LANES = 256
STEP_ROWS = 32


def slot_of_harmonic(harmonic_table):
    slots = jnp.arange(harmonic_table.shape[0], dtype=jnp.int32)
    hit = harmonic_table[:, None] == slots[None, :]
    return jnp.sum(jnp.where(hit, slots[:, None], 0), axis=0)


def real_dft8(x):
    half = math.sqrt(0.5)
    s0, d0 = x[0] + x[4], x[0] - x[4]
    s1, d1 = x[2] + x[6], x[2] - x[6]
    s2, d2 = x[1] + x[5], x[1] - x[5]
    s3, d3 = x[3] + x[7], x[3] - x[7]
    e0, e2 = s0 + s1, s0 - s1
    o0, o2 = s2 + s3, s2 - s3
    t_re, t_im = (d2 - d3) * half, (d2 + d3) * half
    return [
        (e0 + o0, None),
        (d0 + t_re, d1 + t_im),
        (e2, o2),
        (d0 - t_re, t_im - d1),
        (e0 - o0, None),
    ]


def dft4(a, b, c, d):
    s0, d0 = (a[0] + c[0], a[1] + c[1]), (a[0] - c[0], a[1] - c[1])
    s1, d1 = (b[0] + d[0], b[1] + d[1]), (b[0] - d[0], b[1] - d[1])
    return [
        (s0[0] + s1[0], s0[1] + s1[1]),
        (d0[0] - d1[1], d0[1] + d1[0]),
        (s0[0] - s1[0], s0[1] - s1[1]),
        (d0[0] + d1[1], d0[1] - d1[0]),
    ]


def complex_dft8(z):
    half = math.sqrt(0.5)
    even = dft4(z[0], z[2], z[4], z[6])
    odd = dft4(z[1], z[3], z[5], z[7])
    turned = [
        odd[0],
        ((odd[1][0] - odd[1][1]) * half, (odd[1][0] + odd[1][1]) * half),
        (-odd[2][1], odd[2][0]),
        (-(odd[3][0] + odd[3][1]) * half, (odd[3][0] - odd[3][1]) * half),
    ]
    low = [(e[0] + t[0], e[1] + t[1]) for e, t in zip(even, turned)]
    high = [(e[0] - t[0], e[1] - t[1]) for e, t in zip(even, turned)]
    return low + high


def transform_kernel(slot_ref, x_ref, out_ref, mid_ref):
    sectors = 64
    scale = math.sqrt(2.0 / sectors)

    def put(p, re, im):
        at = 2 * slot_ref[p]
        return at, re, im

    for tile in range(STEP_ROWS // 8):
        rows = slice(8 * tile, 8 * tile + 8)

        def store(c, value):
            out_ref[c, rows, :] = value.astype(jnp.bfloat16)

        for s0 in range(8):
            x = []
            for s1 in range(8):
                s = 8 * s1 + s0
                x.append(x_ref[s // 4, s % 4, rows, :].astype(jnp.float32))
            y = real_dft8(x)
            mid_ref[tile, 0, s0] = y[0][0]
            mid_ref[tile, 1, s0] = y[4][0]
            for k1 in range(1, 4):
                mid_ref[tile, 2 * k1, s0] = y[k1][0]
                mid_ref[tile, 2 * k1 + 1, s0] = y[k1][1]
        y = real_dft8([mid_ref[tile, 0, s0] for s0 in range(8)])
        at = 2 * slot_ref[0]
        store(at, y[0][0] * math.sqrt(1.0 / sectors))
        store(at + 1, y[4][0] * math.sqrt(1.0 / sectors))
        for k2 in range(1, 4):
            at = 2 * slot_ref[8 * k2]
            store(at, y[k2][0] * scale)
            store(at + 1, y[k2][1] * scale)
        z = []
        for s0 in range(8):
            angle = 2.0 * math.pi * 4 * s0 / sectors
            value = mid_ref[tile, 1, s0]
            z.append((value * (scale * math.cos(angle)), value * (scale * math.sin(angle))))
        y = complex_dft8(z)
        for k2 in range(4):
            at = 2 * slot_ref[4 + 8 * k2]
            store(at, y[k2][0])
            store(at + 1, y[k2][1])
        for k1 in range(1, 4):
            z = []
            for s0 in range(8):
                angle = 2.0 * math.pi * k1 * s0 / sectors
                c, s = scale * math.cos(angle), scale * math.sin(angle)
                re, im = mid_ref[tile, 2 * k1, s0], mid_ref[tile, 2 * k1 + 1, s0]
                z.append((re * c, im * c) if s0 == 0 else (re * c - im * s, re * s + im * c))
            y = complex_dft8(z)
            for k2 in range(8):
                p = k1 + 8 * k2
                if p < 32:
                    at = 2 * slot_ref[p]
                    store(at, y[k2][0])
                    store(at + 1, y[k2][1])
                else:
                    at = 2 * slot_ref[64 - p]
                    store(at, y[k2][0])
                    store(at + 1, -y[k2][1])


def transform(slots, arrived):
    groups, per, rows, cols = arrived.shape
    spec = pltpu.PrefetchScalarGridSpec(
        num_scalar_prefetch=1,
        grid=(rows // STEP_ROWS,),
        in_specs=[pl.BlockSpec((groups, per, STEP_ROWS, cols), lambda i, s: (0, 0, i, 0))],
        out_specs=pl.BlockSpec((groups * per, STEP_ROWS, cols), lambda i, s: (0, i, 0)),
        scratch_shapes=[pltpu.VMEM((STEP_ROWS // 8, 8, 8, 8, cols), jnp.float32)],
    )
    return pl.pallas_call(
        transform_kernel,
        grid_spec=spec,
        out_shape=jax.ShapeDtypeStruct((groups * per, rows, cols), jnp.bfloat16),
        compiler_params=pltpu.CompilerParams(dimension_semantics=("arbitrary",)),
        cost_estimate=pl.CostEstimate(
            flops=700 * rows * cols, bytes_accessed=4 * groups * per * rows * cols, transcendentals=0
        ),
        name="transform",
    )(slots, arrived)


def band_rows(stiff, mass, h0, h1, h2):
    lhs = jnp.concatenate(
        [jnp.concatenate([r[2] * jnp.bfloat16(0.5), r[3], r[4]], axis=1) for r in (stiff, mass)], axis=0
    )
    parts = []
    for c in range(2):
        rhs = jnp.concatenate([h0[c], h1[c], h2[c]], axis=0)
        parts.append(jnp.dot(lhs, rhs, preferred_element_type=jnp.float32).astype(jnp.bfloat16))
    return parts


def inner_kernel(h_ref, stiff_ref, mass_ref, u_ref, y_ref, pt_ref):
    count = pt_ref.shape[0]

    def body(i, carry):
        rows = pl.ds(i * B, B)
        h0, h1, h2 = h_ref.at[i], h_ref.at[i + 1], h_ref.at[i + 2]
        parts = band_rows(stiff_ref.at[i], mass_ref.at[i], h0, h1, h2)
        for c in range(2):
            y_ref[rows, LANES * c : LANES * (c + 1)] = parts[c][:B]
            y_ref[rows, LANES * (2 + c) : LANES * (3 + c)] = parts[c][B:]
            pt_ref[i, LANES * c : LANES * (c + 1), :] = h0[c].T
        return carry

    lax.fori_loop(0, count, body, 0)
    p_t = jnp.concatenate([pt_ref[i] for i in range(count)], axis=1)
    for n in range(4):
        lanes = slice(LANES * n, LANES * (n + 1))
        u_ref[0, :, lanes] = jnp.dot(p_t, y_ref[:, lanes], preferred_element_type=jnp.float32)


def project_inner(h, stiff, mass):
    blocks, comps = h.shape[:2]
    slots = comps // 2
    count = blocks - REACH
    vmem = pl.BlockSpec(memory_space=pltpu.VMEM)
    return pl.pallas_call(
        inner_kernel,
        grid=(slots,),
        in_specs=[pl.BlockSpec((blocks, 2) + h.shape[2:], lambda s: (0, s, 0, 0)), vmem, vmem],
        out_specs=pl.BlockSpec((1, 2 * LANES, 4 * LANES), lambda s: (s, 0, 0)),
        out_shape=jax.ShapeDtypeStruct((slots, 2 * LANES, 4 * LANES), jnp.float32),
        scratch_shapes=[
            pltpu.VMEM((count * B, 4 * LANES), jnp.bfloat16),
            pltpu.VMEM((count, 2 * LANES, B), jnp.bfloat16),
        ],
        compiler_params=pltpu.CompilerParams(vmem_limit_bytes=28 * 1024 * 1024),
        cost_estimate=pl.CostEstimate(
            flops=slots * count * B * 2 * LANES * (2 * 2 * 3 * B + 2 * 4 * LANES),
            bytes_accessed=2 * (h.size + stiff.size + mass.size),
            transcendentals=0,
        ),
        name="project_inner",
    )(h, stiff, mass)


def last_kernel(h_ref, halo_ref, stiff_ref, mass_ref, u_ref, out_ref, v_ref):
    rows = [h_ref.at[0], h_ref.at[1], halo_ref.at[0], halo_ref.at[1]]
    parts = [band_rows(stiff_ref.at[i], mass_ref.at[i], *rows[i : i + 3]) for i in range(2)]
    p_t = jnp.concatenate(
        [jnp.concatenate([h_ref[i, c].T for c in range(2)], axis=0) for i in range(2)], axis=1
    )
    for n in range(4):
        kind, c = n // 2, n % 2
        lanes = slice(LANES * n, LANES * (n + 1))
        y = jnp.concatenate([parts[i][c][B * kind : B * (kind + 1)] for i in range(2)], axis=0)
        v_ref[:, lanes] = u_ref[0, :, lanes] + jnp.dot(p_t, y, preferred_element_type=jnp.float32)
    high = out_ref.shape[3]
    for kind in range(2):
        base = 2 * LANES * kind
        for q in range(4):
            direct = v_ref[B * q : B * (q + 1), base : base + 2 * LANES]
            mirror = v_ref[:, base + B * q : base + B * (q + 1)].T
            total = (direct + mirror).astype(jnp.bfloat16)
            for part in range(B // high):
                out_ref[q * (B // high) + part, kind, 0] = total[part * high : (part + 1) * high]


def project_last(h, halo, stiff, mass, u, strips):
    blocks, comps = h.shape[:2]
    slots = comps // 2
    at = blocks // REACH - 1
    high = 2 * LANES // strips
    ends = lambda s: (at, 0, 0, 0)
    return pl.pallas_call(
        last_kernel,
        grid=(slots,),
        in_specs=[
            pl.BlockSpec((REACH, 2) + h.shape[2:], lambda s: (at, s, 0, 0)),
            pl.BlockSpec((REACH, 2) + h.shape[2:], lambda s: (0, s, 0, 0)),
            pl.BlockSpec((REACH,) + stiff.shape[1:], ends),
            pl.BlockSpec((REACH,) + mass.shape[1:], ends),
            pl.BlockSpec((1,) + u.shape[1:], lambda s: (s, 0, 0)),
        ],
        out_specs=pl.BlockSpec((strips, 2, 1, high, 2 * LANES), lambda s: (0, 0, s, 0, 0)),
        out_shape=jax.ShapeDtypeStruct((strips, 2, slots, high, 2 * LANES), jnp.bfloat16),
        scratch_shapes=[pltpu.VMEM((2 * LANES, 4 * LANES), jnp.float32)],
        compiler_params=pltpu.CompilerParams(vmem_limit_bytes=20 * 1024 * 1024),
        cost_estimate=pl.CostEstimate(
            flops=slots * REACH * B * 2 * LANES * (2 * 2 * 3 * B + 2 * 4 * LANES),
            bytes_accessed=4 * u.size + 4 * strips * slots * high * 2 * LANES,
            transcendentals=0,
        ),
        name="project_last",
    )(h, halo, stiff, mass, u)


def per_device(psi_sectors, stiff_blocks, mass_blocks, harmonic_table):
    sec_dev, rows_dev, cols = psi_sectors.shape
    sector_count = lax.axis_size("sector")
    row_count = lax.axis_size("row")
    blocks = rows_dev // B
    pieces = psi_sectors.reshape(sec_dev, sector_count, rows_dev // sector_count, cols)
    pieces = jnp.swapaxes(pieces, 0, 1)
    arrived = lax.all_to_all(pieces, "sector", 0, 0, tiled=True)
    components = transform(slot_of_harmonic(harmonic_table), arrived)
    outgoing = components.reshape(sector_count, sec_dev, rows_dev // sector_count, cols)
    h = lax.all_to_all(outgoing, "sector", 0, 0, tiled=True)
    h = h.reshape(sector_count, sec_dev, -1, B, cols)
    h = jnp.swapaxes(h, 1, 2).reshape(blocks, sec_dev, B, cols)
    backward = [(i + 1, i) for i in range(row_count - 1)]
    halo = lax.ppermute(h[:REACH], "row", backward)
    u = project_inner(h, stiff_blocks, mass_blocks)
    parts = project_last(h, halo, stiff_blocks, mass_blocks, u, row_count)
    arrived_parts = lax.all_to_all(parts, "row", 0, 0, tiled=True)
    total = jnp.sum(arrived_parts.astype(jnp.float32), axis=0)
    return total[0], total[1]


def solution(mesh):
    placed = (P("sector", "row", None), P("row", None, None, None), P("row", None, None, None), P())
    return jax.shard_map(
        per_device,
        mesh=mesh,
        in_specs=placed,
        out_specs=(P("sector", "row", None), P("sector", "row", None)),
        check_vma=False,
    )
```
